32 devices in a mesh: fsdp: 16 (over z, y, x), dp: 2 (over core).
Axes of the slice: x: 2, y: 2, z: 4, core: 2. Of those that a mesh axis runs over, the one named last changes fastest.
Arguments:
- normed: bfloat16 [2, 4096, 4096], P(None, ('fsdp', 'dp')), may hold values from -6 to 6
- kv_cotangent: bfloat16 [2, 4096, 512], P(None, ('fsdp', 'dp')), may hold values from -6 to 6
- kv_weight: bfloat16 [4096, 512], P('fsdp'), may hold values from -0.09375 to 0.09375
- main_grad: float32 [4096, 512], P('fsdp'), may hold values from -6 to 6
- owner_order: int32 [16], replicated, may hold values from 0 to 15, each once
Outputs:
- key_rows: bfloat16 [2, 4096, 512], P(None, ('fsdp', 'dp'))
- input_grad: bfloat16 [2, 4096, 4096], P(None, ('fsdp', 'dp'))
- grad_buffer: float32 [4096, 512], P('fsdp')
The draws below stay inside these ranges and needn't reach their ends.
Inputs may be any that keep to these rules, and one draw needn't show every extreme that they name: `owner_order`: a permutation: each value appears once.
All inputs are finite; a program needn't handle non-finite values.
Results may differ from the reference program's by a relative error of at most 0.0075.
Values may be sent and summed in bfloat16 or wider, within the bound.
A program may use at most 64 MiB of HBM per device.

```python
import math
import jax
import jax.numpy as jnp
from jax import lax

D = 4096
MICRO = 2
TOK_DEV = 128
KVW = 512
TOKENS = 4096
N_FSDP = 16
N_DP = 2


def steps_of(rng, dims, split, smallest, high):
    level = 1.0
    for axis_at, blocks in split:
        heights = jax.random.uniform(jax.random.fold_in(jax.random.fold_in(rng, 6), axis_at), (blocks,), jnp.float32, smallest / len(split), high / len(split))
        level = level * jnp.repeat(jnp.exp(heights), dims[axis_at] // blocks).reshape((-1,) + (1,) * (len(dims) - 1 - axis_at))
    return level


def gaussian(rng, shape, scale, reach, cuts=(), kind=jnp.bfloat16):
    level = steps_of(rng, shape, cuts, -0.22, 0.18) if cuts else 1.0
    array = jax.random.normal(rng, shape, jnp.float32) * scale * level
    return jnp.minimum(jnp.maximum(array, -reach), reach).astype(kind)


def setup_inputs(seed: int = 0) -> dict:
    key_list = jax.random.split(jax.random.key(seed), 6)
    normed = gaussian(key_list[0], (MICRO, TOKENS, D), 1.0, 6.0, ((1, 32),))
    kv_cotangent = gaussian(key_list[1], (MICRO, TOKENS, KVW), 1.0, 6.0, ((1, 32),))
    kv_weight = gaussian(key_list[2], (D, KVW), D ** -0.5, 0.09375, ((0, 16),))
    main_grad = gaussian(key_list[3], (D, KVW), 1.0, 6.0, ((0, 16),), jnp.float32)
    owner_order = jax.random.permutation(key_list[4], N_FSDP).astype(jnp.int32)
    return dict(normed=normed, kv_cotangent=kv_cotangent, kv_weight=kv_weight, main_grad=main_grad, owner_order=owner_order)


def reference(normed, kv_cotangent, kv_weight, main_grad, owner_order):
    shard_rows = D // N_FSDP
    block_count = MICRO * N_DP
    block_rows = TOK_DEV * N_FSDP
    inverse_owner = jnp.argsort(owner_order).astype(jnp.int32)
    blocks_in = normed.reshape(block_count, block_rows, D)
    blocks_cot = kv_cotangent.reshape(block_count, block_rows, KVW)

    def advance(grad_sum, inputs_pair):
        inputs, cotangent = inputs_pair
        permuted = inputs.reshape(block_rows, N_FSDP, shard_rows)[:, owner_order, :].reshape(block_rows, D)
        key_block = jnp.dot(permuted, kv_weight, preferred_element_type=jnp.float32).astype(jnp.bfloat16)
        grad_permuted = jnp.dot(cotangent, kv_weight.T, preferred_element_type=jnp.float32).astype(jnp.bfloat16)
        grad_block = grad_permuted.reshape(block_rows, N_FSDP, shard_rows)[:, inverse_owner, :].reshape(block_rows, D)
        grad_sum = grad_sum + jnp.dot(permuted.T, cotangent, preferred_element_type=jnp.float32)
        return (grad_sum, (key_block, grad_block))
    grad_sum, outputs = lax.scan(advance, jnp.zeros((D, KVW), jnp.float32), (blocks_in, blocks_cot))
    key_blocks, grad_blocks = outputs
    grad_scale = 1.0 / math.sqrt(MICRO * TOKENS)
    grad_buffer = main_grad + grad_sum * grad_scale
    return (key_blocks.reshape(MICRO, TOKENS, KVW), grad_blocks.reshape(MICRO, TOKENS, D), grad_buffer)
```

```python
import functools
import math

import jax
import jax.numpy as jnp
from jax import lax
from jax.experimental import pallas as pl
from jax.experimental.pallas import tpu as pltpu
from jax.sharding import PartitionSpec as P

MESH = pl.DeviceIdType.MESH
F32 = jnp.float32
BF16 = jnp.bfloat16


def kernel(
    n, dp, chunk, scale,
    x_hbm, c_hbm, w_hbm, main_hbm,
    key_hbm, ig_hbm, gb_hbm,
    xx, cc, ck, gath, part, r1, t1, r2, t2, r3, fin, main, gb, key, ig,
    load_sem, out_sem, send_sem, x_recv, az_recv, a1_recv, a2_recv, ad_recv, r1_recv, r2_recv, r3_recv, rd_recv,
):
    f = lax.axis_index("fsdp")
    d = lax.axis_index("dp")
    k = lax.rem(d, 2)
    sib = d + 1 - 2 * k
    rows, width = x_hbm.shape
    key_width = c_hbm.shape[1]
    half = key_width // 2
    depth = n // 4
    chunks = width // chunk
    z = lax.div(f, 4)
    low = lax.rem(f, 4)
    bit0 = lax.rem(low, 2)
    bit1 = lax.div(low, 2)
    flip_x = low + 1 - 2 * bit0
    flip_y = low + 2 - 4 * bit1
    low1 = flip_x + k * (flip_y - flip_x)
    low2 = flip_y + k * (flip_x - flip_y)
    low12 = 3 - low
    p1 = z * 4 + low1
    p2 = z * 4 + low2
    steps = sorted(range(1, depth), key=lambda s: (min(s, depth - s), s))

    def peer(s):
        return lax.rem(z + s, depth)

    def dev(fi, di):
        return {"fsdp": fi, "dp": di}

    loads = []

    def load(src, dst, i):
        cp = pltpu.make_async_copy(src, dst, load_sem.at[i])
        cp.start()
        loads.append(cp)

    load(w_hbm.at[:, pl.ds(0, half)], gath.at[0, f], 0)
    load(w_hbm.at[:, pl.ds(half, half)], gath.at[1, f], 1)
    load(c_hbm, cc.at[0], 2)
    load(x_hbm, xx.at[0], 3)
    load(main_hbm, main, 4)

    barrier = pltpu.get_barrier_semaphore()
    greeted = [dev(peer(s) * 4 + low, d) for s in steps]
    greeted += [dev(p1, d), dev(p2, d)]
    greeted += [dev(f, lax.rem(d + s, dp)) for s in range(1, dp)]
    for g in greeted:
        pl.semaphore_signal(barrier, inc=1, device_id=g, device_id_type=MESH)
    pl.semaphore_wait(barrier, len(greeted))

    sent = []

    def send(src, dst, rsem, to):
        cp = pltpu.make_async_remote_copy(
            src_ref=src, dst_ref=dst, send_sem=send_sem, recv_sem=rsem, device_id=to, device_id_type=MESH
        )
        cp.start()
        sent.append(cp)

    def arrived(dst, rsem, frm):
        pltpu.make_async_remote_copy(
            src_ref=dst, dst_ref=dst, send_sem=send_sem, recv_sem=rsem, device_id=frm, device_id_type=MESH
        ).wait_recv()

    to_sib = dev(f, sib)
    to1 = dev(p1, d)
    to2 = dev(p2, d)

    send(x_hbm, xx.at[1], x_recv.at[0], to_sib)
    send(c_hbm, cc.at[1], x_recv.at[1], to_sib)
    loads[0].wait()
    loads[1].wait()

    def block(fi):
        return gath.at[k, fi]

    send(block(f), block(f), a1_recv.at[z], to1)
    send(block(f), block(f), a2_recv.at[z], to2)
    for s in steps:
        send(block(f), block(f), az_recv.at[z], dev(peer(s) * 4 + low, d))

    loads[2].wait()
    loads[3].wait()
    arrived(cc.at[1], x_recv.at[1], to_sib)
    arrived(xx.at[1], x_recv.at[0], to_sib)
    side = pl.ds(pl.multiple_of(k * half, half), half)
    ck[...] = cc[:, :, side].reshape(2 * rows, half)

    per = chunk // part.shape[1]
    for j in range(chunks):
        both = xx[:, :, j * chunk : (j + 1) * chunk].reshape(2 * rows, chunk)
        prod = lax.dot_general(both, ck[...], (((0,), (0,)), ((), ())), preferred_element_type=F32)
        part[j * per : (j + 1) * per] = prod.astype(BF16).reshape(per, part.shape[1], half)

    ring = steps + [0]
    for s in ring:
        send(part.at[peer(s) * 4 + low12], r1.at[0, peer(s)], r1_recv.at[0, peer(s)], to1)
    for s in steps:
        zb = peer(s)
        fb = zb * 4 + low
        arrived(block(fb), az_recv.at[zb], dev(fb, d))
        send(block(fb), block(fb), a1_recv.at[zb], to1)
        send(block(fb), block(fb), a2_recv.at[zb], to2)
        send(block(fb), block(fb), ad_recv.at[fb], to_sib)
    for s in ring:
        send(part.at[peer(s) * 4 + low1], r1.at[1, peer(s)], r1_recv.at[1, peer(s)], to1)
    for s in [0] + steps:
        zb = peer(s)
        fb = zb * 4 + low1
        arrived(block(fb), a1_recv.at[zb], to1)
        send(block(fb), block(fb), a2_recv.at[depth + zb], to2)
        send(block(fb), block(fb), ad_recv.at[fb], to_sib)
    for s in ring:
        zb = peer(s)
        arrived(r1.at[0, zb], r1_recv.at[0, zb], to1)
        t1[zb] = (part[zb * 4 + low2].astype(F32) + r1[0, zb].astype(F32)).astype(BF16)
        send(t1.at[zb], r2.at[zb], r2_recv.at[zb], to2)
    for s in steps:
        zb = peer(s)
        arrived(r1.at[1, zb], r1_recv.at[1, zb], to1)
        arrived(r2.at[zb], r2_recv.at[zb], to2)
        t2[zb] = (part[zb * 4 + low].astype(F32) + r1[1, zb].astype(F32) + r2[zb].astype(F32)).astype(BF16)
        send(t2.at[zb], r3.at[z], r3_recv.at[z], dev(zb * 4 + low, d))
    for s in [0] + steps:
        zb = peer(s)
        fb = zb * 4 + low2
        arrived(block(fb), a2_recv.at[zb], to2)
        send(block(fb), block(fb), ad_recv.at[fb], to_sib)
    for s in [0] + steps:
        zb = peer(s)
        fb = zb * 4 + low12
        arrived(block(fb), a2_recv.at[depth + zb], to2)
        send(block(fb), block(fb), ad_recv.at[fb], to_sib)

    arrived(r1.at[1, z], r1_recv.at[1, z], to1)
    arrived(r2.at[z], r2_recv.at[z], to2)
    total = part[f].astype(F32) + r1[1, z].astype(F32) + r2[z].astype(F32)
    for s in steps:
        arrived(r3.at[peer(s)], r3_recv.at[peer(s)], dev(peer(s) * 4 + low, d))
        total = total + r3[peer(s)].astype(F32)
    fin[d] = total
    for s in range(1, dp):
        send(fin.at[d], fin.at[d], rd_recv.at[d], dev(f, lax.rem(d + s, dp)))

    for s in [0] + steps:
        for lo in (low, low1, low2, low12):
            if s == 0 and lo is low:
                continue
            fb = peer(s) * 4 + lo
            arrived(gath.at[1 - k, fb], ad_recv.at[fb], to_sib)

    outs = []

    def put(src, dst, i):
        cp = pltpu.make_async_copy(src, dst, out_sem.at[i])
        cp.start()
        outs.append(cp)

    group = max(1, chunks // 4)
    for j in range(chunks):
        w0 = gath[0, j * per : (j + 1) * per].reshape(chunk, half)
        w1 = gath[1, j * per : (j + 1) * per].reshape(chunk, half)
        contract = (((1,), (1,)), ((), ()))
        prod = lax.dot_general(cc[0, :, :half], w0, contract, preferred_element_type=F32)
        prod = prod + lax.dot_general(cc[0, :, half:], w1, contract, preferred_element_type=F32)
        ig[:, j * chunk : (j + 1) * chunk] = prod.astype(BF16)
        if (j + 1) % group == 0:
            cols = pl.ds((j + 1 - group) * chunk, group * chunk)
            put(ig.at[:, cols], ig_hbm.at[:, cols], (j + 1) // group - 1)
    for h in range(2):
        w = gath[h].reshape(width, half)
        key[:, h * half : (h + 1) * half] = jnp.dot(xx[0], w, preferred_element_type=F32).astype(BF16)
    put(key, key_hbm, chunks // group)

    for s in range(1, dp):
        src = lax.rem(d + s, dp)
        arrived(fin.at[src], rd_recv.at[src], dev(f, src))
    loads[4].wait()
    for h in range(2):
        total = fin[h]
        for g in range(1, dp // 2):
            total = total + fin[2 * g + h]
        cols = slice(h * half, (h + 1) * half)
        gb[:, cols] = main[:, cols] + total * scale
    put(gb, gb_hbm, chunks // group + 1)
    for cp in sent:
        cp.wait_send()
    for cp in outs:
        cp.wait()


def reorder_kernel(depth, scatter, order_ref, x_ref, y_ref):
    for j in range(x_ref.shape[1] // depth):
        here = slice(j * depth, (j + 1) * depth)
        there = pl.ds(pl.multiple_of(order_ref[j] * depth, depth), depth)
        if scatter:
            y_ref[:, there] = x_ref[:, here]
        else:
            y_ref[:, here] = x_ref[:, there]


def reorder(x, order, scatter):
    rows, width = x.shape
    n = order.shape[0]
    depth = width // n
    if depth % 128:
        if scatter:
            order = jnp.argsort(order)
        return jnp.take(x.reshape(rows, n, depth), order, axis=1, mode="clip").reshape(rows, width)
    tile = rows // 4
    spec = pl.BlockSpec((tile, width), lambda i: (i, 0))
    return pl.pallas_call(
        functools.partial(reorder_kernel, depth, scatter),
        grid=(rows // tile,),
        out_shape=jax.ShapeDtypeStruct((rows, width), x.dtype),
        in_specs=[pl.BlockSpec(memory_space=pltpu.SMEM), spec],
        out_specs=spec,
        cost_estimate=pl.CostEstimate(flops=0, bytes_accessed=4 * rows * width, transcendentals=0),
    )(order, x)


def body(normed, kv_cotangent, kv_weight, main_grad, owner_order):
    micro_count, tok_dev, width = normed.shape
    shard_rows, key_width = kv_weight.shape
    n = lax.axis_size("fsdp")
    dp = lax.axis_size("dp")
    rows = micro_count * tok_dev
    half = key_width // 2
    depth = n // 4
    scale = 1.0 / math.sqrt(rows * n * dp)
    chunk = max(shard_rows, 256)
    x = reorder(normed.reshape(rows, width), owner_order, False)
    chunks = width // chunk
    dma = pltpu.SemaphoreType.DMA
    half_block = (shard_rows, half)
    any_spec = pl.BlockSpec(memory_space=pl.ANY)
    key, ig, gb = pl.pallas_call(
        functools.partial(kernel, n, dp, chunk, scale),
        out_shape=(
            jax.ShapeDtypeStruct((rows, key_width), BF16),
            jax.ShapeDtypeStruct((rows, width), BF16),
            jax.ShapeDtypeStruct((shard_rows, key_width), F32),
        ),
        in_specs=[any_spec] * 4,
        out_specs=(any_spec,) * 3,
        scratch_shapes=[
            pltpu.VMEM((2, rows, width), BF16),
            pltpu.VMEM((2, rows, key_width), BF16),
            pltpu.VMEM((2 * rows, half), BF16),
            pltpu.VMEM((2, n) + half_block, BF16),
            pltpu.VMEM((n,) + half_block, BF16),
            pltpu.VMEM((2, depth) + half_block, BF16),
            pltpu.VMEM((depth,) + half_block, BF16),
            pltpu.VMEM((depth,) + half_block, BF16),
            pltpu.VMEM((depth,) + half_block, BF16),
            pltpu.VMEM((depth,) + half_block, BF16),
            pltpu.VMEM((dp,) + half_block, F32),
            pltpu.VMEM((shard_rows, key_width), F32),
            pltpu.VMEM((shard_rows, key_width), F32),
            pltpu.VMEM((rows, key_width), BF16),
            pltpu.VMEM((rows, width), BF16),
            dma((5,)),
            dma((chunks // max(1, chunks // 4) + 2,)),
            dma,
            dma((2,)),
            dma((depth,)),
            dma((depth,)),
            dma((2 * depth,)),
            dma((n,)),
            dma((2, depth)),
            dma((depth,)),
            dma((depth,)),
            dma((dp,)),
        ],
        compiler_params=pltpu.CompilerParams(
            collective_id=0, has_side_effects=True
        ),
    )(x, kv_cotangent.reshape(rows, key_width), kv_weight, main_grad)
    ig = reorder(ig, owner_order, True)
    return (
        key.reshape(micro_count, tok_dev, key_width),
        ig.reshape(micro_count, tok_dev, width),
        gb,
    )


def solution(mesh):
    in_specs = (
        P(None, ("fsdp", "dp"), None),
        P(None, ("fsdp", "dp"), None),
        P("fsdp", None),
        P("fsdp", None),
        P(),
    )
    out_specs = (P(None, ("fsdp", "dp"), None), P(None, ("fsdp", "dp"), None), P("fsdp", None))
    return jax.shard_map(body, mesh=mesh, in_specs=in_specs, out_specs=out_specs, check_vma=False)
```

```python
import functools
import math

import jax
import jax.numpy as jnp
from jax import lax
from jax.experimental import pallas as pl
from jax.experimental.pallas import tpu as pltpu
from jax.sharding import PartitionSpec as P

MESH = pl.DeviceIdType.MESH
F32 = jnp.float32
BF16 = jnp.bfloat16


def kernel(
    n, dp, chunk, scale,
    x_hbm, c_hbm, w_hbm, main_hbm,
    key_hbm, ig_hbm, gb_hbm,
    xx, cc, ck, gath, part, r1, t1, r2, t2, r3, fin, main, gb, key, ig, acc,
    load_sem, out_sem, send_sem, x_recv, az_recv, a1_recv, a2_recv, ad_recv, r1_recv, r2_recv, r3_recv, rd_recv,
):
    f = lax.axis_index("fsdp")
    d = lax.axis_index("dp")
    k = lax.rem(d, 2)
    sib = d + 1 - 2 * k
    rows, width = x_hbm.shape
    key_width = c_hbm.shape[1]
    half = key_width // 2
    depth = n // 4
    chunks = width // chunk
    z = lax.div(f, 4)
    low = lax.rem(f, 4)
    bit0 = lax.rem(low, 2)
    bit1 = lax.div(low, 2)
    flip_x = low + 1 - 2 * bit0
    flip_y = low + 2 - 4 * bit1
    low1 = flip_x + k * (flip_y - flip_x)
    low2 = flip_y + k * (flip_x - flip_y)
    low12 = 3 - low
    p1 = z * 4 + low1
    p2 = z * 4 + low2
    steps = sorted(range(1, depth), key=lambda s: (min(s, depth - s), s))

    def peer(s):
        return lax.rem(z + s, depth)

    def dev(fi, di):
        return {"fsdp": fi, "dp": di}

    loads = []

    def load(src, dst, i):
        cp = pltpu.make_async_copy(src, dst, load_sem.at[i])
        cp.start()
        loads.append(cp)

    load(w_hbm.at[:, pl.ds(0, half)], gath.at[0, f], 0)
    load(w_hbm.at[:, pl.ds(half, half)], gath.at[1, f], 1)
    load(c_hbm, cc.at[0], 2)
    load(x_hbm, xx.at[0], 3)
    load(main_hbm, main, 4)

    barrier = pltpu.get_barrier_semaphore()
    greeted = [dev(peer(s) * 4 + low, d) for s in steps]
    greeted += [dev(p1, d), dev(p2, d)]
    greeted += [dev(f, lax.rem(d + s, dp)) for s in range(1, dp)]
    for g in greeted:
        pl.semaphore_signal(barrier, inc=1, device_id=g, device_id_type=MESH)
    pl.semaphore_wait(barrier, len(greeted))

    sent = []

    def send(src, dst, rsem, to):
        cp = pltpu.make_async_remote_copy(
            src_ref=src, dst_ref=dst, send_sem=send_sem, recv_sem=rsem, device_id=to, device_id_type=MESH
        )
        cp.start()
        sent.append(cp)

    def arrived(dst, rsem, frm):
        pltpu.make_async_remote_copy(
            src_ref=dst, dst_ref=dst, send_sem=send_sem, recv_sem=rsem, device_id=frm, device_id_type=MESH
        ).wait_recv()

    to_sib = dev(f, sib)
    to1 = dev(p1, d)
    to2 = dev(p2, d)

    send(x_hbm, xx.at[1], x_recv.at[0], to_sib)
    send(c_hbm, cc.at[1], x_recv.at[1], to_sib)
    loads[0].wait()
    loads[1].wait()

    def block(fi):
        return gath.at[k, fi]

    send(block(f), block(f), a1_recv.at[z], to1)
    send(block(f), block(f), a2_recv.at[z], to2)
    for s in steps:
        send(block(f), block(f), az_recv.at[z], dev(peer(s) * 4 + low, d))

    loads[2].wait()
    loads[3].wait()
    arrived(cc.at[1], x_recv.at[1], to_sib)
    arrived(xx.at[1], x_recv.at[0], to_sib)
    side = pl.ds(pl.multiple_of(k * half, half), half)
    ck[...] = cc[:, :, side].reshape(2 * rows, half)

    per = chunk // part.shape[1]
    ring = steps + [0]
    blockwise = per == 1

    def partial(cols):
        both = xx[:, :, cols].reshape(2 * rows, chunk)
        prod = lax.dot_general(both, ck[...], (((0,), (0,)), ((), ())), preferred_element_type=F32)
        return prod.astype(BF16)

    def feature_block(fb):
        return pl.ds(pl.multiple_of(fb * chunk, chunk), chunk)

    def partials(lo):
        if blockwise:
            for s in ring:
                fb = peer(s) * 4 + lo
                part[fb] = partial(feature_block(fb))
                if lo is low12:
                    send(part.at[fb], r1.at[0, peer(s)], r1_recv.at[0, peer(s)], to1)
                if lo is low1:
                    send(part.at[fb], r1.at[1, peer(s)], r1_recv.at[1, peer(s)], to1)

    if not blockwise:
        for j in range(chunks):
            made = partial(pl.ds(j * chunk, chunk))
            part[j * per : (j + 1) * per] = made.reshape(per, part.shape[1], half)
        for s in ring:
            send(part.at[peer(s) * 4 + low12], r1.at[0, peer(s)], r1_recv.at[0, peer(s)], to1)
    partials(low12)
    for s in steps:
        zb = peer(s)
        fb = zb * 4 + low
        arrived(block(fb), az_recv.at[zb], dev(fb, d))
        send(block(fb), block(fb), a1_recv.at[zb], to1)
        send(block(fb), block(fb), a2_recv.at[zb], to2)
        send(block(fb), block(fb), ad_recv.at[fb], to_sib)
    if not blockwise:
        for s in ring:
            send(part.at[peer(s) * 4 + low1], r1.at[1, peer(s)], r1_recv.at[1, peer(s)], to1)
    partials(low1)
    partials(low2)
    partials(low)

    outs = []

    def put(src, dst, i):
        cp = pltpu.make_async_copy(src, dst, out_sem.at[i])
        cp.start()
        outs.append(cp)

    contract = (((1,), (1,)), ((), ()))

    def from_sib(lo):
        for s in [0] + steps:
            fb = peer(s) * 4 + lo
            if s or lo is not low:
                arrived(gath.at[1 - k, fb], ad_recv.at[fb], to_sib)

    def use(lo):
        if not blockwise:
            return
        from_sib(lo)
        for s in [0] + steps:
            fb = peer(s) * 4 + lo
            cols = feature_block(fb)
            w0 = gath[0, fb]
            w1 = gath[1, fb]
            prod = lax.dot_general(cc[0, :, :half], w0, contract, preferred_element_type=F32)
            prod = prod + lax.dot_general(cc[0, :, half:], w1, contract, preferred_element_type=F32)
            ig[:, cols] = prod.astype(BF16)
            put(ig.at[:, cols], ig_hbm.at[:, cols], len(outs))
            xb = xx[0, :, cols]
            k0 = jnp.dot(xb, w0, preferred_element_type=F32)
            k1 = jnp.dot(xb, w1, preferred_element_type=F32)
            if s == 0 and lo is low:
                acc[:, :half] = k0
                acc[:, half:] = k1
            else:
                acc[:, :half] += k0
                acc[:, half:] += k1

    for s in [0] + steps:
        zb = peer(s)
        fb = zb * 4 + low1
        arrived(block(fb), a1_recv.at[zb], to1)
        send(block(fb), block(fb), a2_recv.at[depth + zb], to2)
        send(block(fb), block(fb), ad_recv.at[fb], to_sib)
    for s in ring:
        zb = peer(s)
        arrived(r1.at[0, zb], r1_recv.at[0, zb], to1)
        t1[zb] = (part[zb * 4 + low2].astype(F32) + r1[0, zb].astype(F32)).astype(BF16)
        send(t1.at[zb], r2.at[zb], r2_recv.at[zb], to2)
    use(low)
    for s in steps:
        zb = peer(s)
        arrived(r1.at[1, zb], r1_recv.at[1, zb], to1)
        arrived(r2.at[zb], r2_recv.at[zb], to2)
        t2[zb] = (part[zb * 4 + low].astype(F32) + r1[1, zb].astype(F32) + r2[zb].astype(F32)).astype(BF16)
        send(t2.at[zb], r3.at[z], r3_recv.at[z], dev(zb * 4 + low, d))
    for s in [0] + steps:
        zb = peer(s)
        fb = zb * 4 + low2
        arrived(block(fb), a2_recv.at[zb], to2)
        send(block(fb), block(fb), ad_recv.at[fb], to_sib)
    use(low1)
    use(low2)
    for s in [0] + steps:
        zb = peer(s)
        fb = zb * 4 + low12
        arrived(block(fb), a2_recv.at[depth + zb], to2)
        send(block(fb), block(fb), ad_recv.at[fb], to_sib)

    arrived(r1.at[1, z], r1_recv.at[1, z], to1)
    arrived(r2.at[z], r2_recv.at[z], to2)
    total = part[f].astype(F32) + r1[1, z].astype(F32) + r2[z].astype(F32)
    for s in steps:
        arrived(r3.at[peer(s)], r3_recv.at[peer(s)], dev(peer(s) * 4 + low, d))
        total = total + r3[peer(s)].astype(F32)
    fin[d] = total
    for s in range(1, dp):
        send(fin.at[d], fin.at[d], rd_recv.at[d], dev(f, lax.rem(d + s, dp)))

    use(low12)
    if blockwise:
        key[...] = acc[...].astype(BF16)
    else:
        for lo in (low, low1, low2, low12):
            from_sib(lo)
        for j in range(chunks):
            w0 = gath[0, j * per : (j + 1) * per].reshape(chunk, half)
            w1 = gath[1, j * per : (j + 1) * per].reshape(chunk, half)
            prod = lax.dot_general(cc[0, :, :half], w0, contract, preferred_element_type=F32)
            prod = prod + lax.dot_general(cc[0, :, half:], w1, contract, preferred_element_type=F32)
            ig[:, j * chunk : (j + 1) * chunk] = prod.astype(BF16)
        put(ig, ig_hbm, 0)
        for h in range(2):
            w = gath[h].reshape(width, half)
            key[:, h * half : (h + 1) * half] = jnp.dot(xx[0], w, preferred_element_type=F32).astype(BF16)
    put(key, key_hbm, len(outs))

    for s in range(1, dp):
        src = lax.rem(d + s, dp)
        arrived(fin.at[src], rd_recv.at[src], dev(f, src))
    loads[4].wait()
    for h in range(2):
        total = fin[h]
        for g in range(1, dp // 2):
            total = total + fin[2 * g + h]
        cols = slice(h * half, (h + 1) * half)
        gb[:, cols] = main[:, cols] + total * scale
    put(gb, gb_hbm, len(outs))
    for cp in sent:
        cp.wait_send()
    for cp in outs:
        cp.wait()


def reorder_kernel(depth, scatter, order_ref, x_ref, y_ref):
    for j in range(x_ref.shape[1] // depth):
        here = slice(j * depth, (j + 1) * depth)
        there = pl.ds(pl.multiple_of(order_ref[j] * depth, depth), depth)
        if scatter:
            y_ref[:, there] = x_ref[:, here]
        else:
            y_ref[:, here] = x_ref[:, there]


def reorder(x, order, scatter):
    rows, width = x.shape
    n = order.shape[0]
    depth = width // n
    if depth % 128:
        if scatter:
            order = jnp.argsort(order)
        return jnp.take(x.reshape(rows, n, depth), order, axis=1, mode="clip").reshape(rows, width)
    tile = rows // 4
    spec = pl.BlockSpec((tile, width), lambda i: (i, 0))
    return pl.pallas_call(
        functools.partial(reorder_kernel, depth, scatter),
        grid=(rows // tile,),
        out_shape=jax.ShapeDtypeStruct((rows, width), x.dtype),
        in_specs=[pl.BlockSpec(memory_space=pltpu.SMEM), spec],
        out_specs=spec,
        cost_estimate=pl.CostEstimate(flops=0, bytes_accessed=4 * rows * width, transcendentals=0),
    )(order, x)


def body(normed, kv_cotangent, kv_weight, main_grad, owner_order):
    micro_count, tok_dev, width = normed.shape
    shard_rows, key_width = kv_weight.shape
    n = lax.axis_size("fsdp")
    dp = lax.axis_size("dp")
    rows = micro_count * tok_dev
    half = key_width // 2
    depth = n // 4
    scale = 1.0 / math.sqrt(rows * n * dp)
    chunk = shard_rows if shard_rows % 128 == 0 else max(shard_rows, 256)
    x = reorder(normed.reshape(rows, width), owner_order, False)
    chunks = width // chunk
    dma = pltpu.SemaphoreType.DMA
    half_block = (shard_rows, half)
    any_spec = pl.BlockSpec(memory_space=pl.ANY)
    key, ig, gb = pl.pallas_call(
        functools.partial(kernel, n, dp, chunk, scale),
        out_shape=(
            jax.ShapeDtypeStruct((rows, key_width), BF16),
            jax.ShapeDtypeStruct((rows, width), BF16),
            jax.ShapeDtypeStruct((shard_rows, key_width), F32),
        ),
        in_specs=[any_spec] * 4,
        out_specs=(any_spec,) * 3,
        scratch_shapes=[
            pltpu.VMEM((2, rows, width), BF16),
            pltpu.VMEM((2, rows, key_width), BF16),
            pltpu.VMEM((2 * rows, half), BF16),
            pltpu.VMEM((2, n) + half_block, BF16),
            pltpu.VMEM((n,) + half_block, BF16),
            pltpu.VMEM((2, depth) + half_block, BF16),
            pltpu.VMEM((depth,) + half_block, BF16),
            pltpu.VMEM((depth,) + half_block, BF16),
            pltpu.VMEM((depth,) + half_block, BF16),
            pltpu.VMEM((depth,) + half_block, BF16),
            pltpu.VMEM((dp,) + half_block, F32),
            pltpu.VMEM((shard_rows, key_width), F32),
            pltpu.VMEM((shard_rows, key_width), F32),
            pltpu.VMEM((rows, key_width), BF16),
            pltpu.VMEM((rows, width), BF16),
            pltpu.VMEM((rows, key_width), F32),
            dma((5,)),
            dma((chunks + 2,)),
            dma,
            dma((2,)),
            dma((depth,)),
            dma((depth,)),
            dma((2 * depth,)),
            dma((n,)),
            dma((2, depth)),
            dma((depth,)),
            dma((depth,)),
            dma((dp,)),
        ],
        compiler_params=pltpu.CompilerParams(
            collective_id=0, has_side_effects=True
        ),
    )(x, kv_cotangent.reshape(rows, key_width), kv_weight, main_grad)
    ig = reorder(ig, owner_order, True)
    return (
        key.reshape(micro_count, tok_dev, key_width),
        ig.reshape(micro_count, tok_dev, width),
        gb,
    )


def solution(mesh):
    in_specs = (
        P(None, ("fsdp", "dp"), None),
        P(None, ("fsdp", "dp"), None),
        P("fsdp", None),
        P("fsdp", None),
        P(),
    )
    out_specs = (P(None, ("fsdp", "dp"), None), P(None, ("fsdp", "dp"), None), P("fsdp", None))
    return jax.shard_map(body, mesh=mesh, in_specs=in_specs, out_specs=out_specs, check_vma=False)
```
